256 devices in a mesh: dp: 16 (over z_hi, x), tp: 16 (over z_lo, y, core).
Axes of the slice: x: 4, y: 4, z: 8 (z_hi: 4, z_lo: 2; z = z_hi * 2 + z_lo), core: 2. Of those that a mesh axis runs over, the one named last changes fastest.
Arguments:
- gradients: bfloat16 [16, 4, 5120, 1280], P('dp', None, 'tp'), may hold values from -6 to 6
- right_factor: float32 [4, 1280, 32], replicated, may hold values from -6 to 6
- weights_before: float32 [4, 5120, 1280], P(None, 'tp', 'dp'), may hold values from -0.15625 to 0.15625
- momentum: float32 [4, 5120, 1280], P(None, 'tp', 'dp'), may hold values from -0.3125 to 0.3125
Outputs:
- new_weights: float32 [4, 5120, 1280], P(None, 'tp', 'dp')
- new_basis: float32 [4, 1280, 32], replicated
- new_momentum: float32 [4, 5120, 1280], P(None, 'tp', 'dp')
The draws below stay inside these ranges and needn't reach their ends.
All inputs are finite; a program needn't handle non-finite values.
Results may differ from the reference program's by a relative error of at most 0.003.
Values sent between devices are 32-bit elements; how exact they have to be, the bound alone decides.
A program may use at most 64 MiB of HBM per device.

```python
import jax
import jax.numpy as jnp
from jax import lax

WIDTH = 1280
INNER = 5120
RANK = 32
LAYERS = 4
REPLICAS = 16
N_TP = 16


def draw_gradients(key, part):
    keys = jax.random.split(key, 5)
    level = jnp.exp(jax.random.uniform(keys[4], (1, LAYERS, N_TP, 1, RANK), jnp.float32, -1.3, 1.3))
    left = jax.random.normal(keys[0], (1, LAYERS, N_TP, INNER // N_TP, RANK), jnp.float32) * level
    left = left.reshape(1, LAYERS, INNER, RANK)
    right = jax.random.normal(keys[1], (1, LAYERS, RANK, WIDTH), jnp.float32)
    strength = jax.random.normal(keys[2], (REPLICAS, LAYERS, 1, RANK), jnp.float32)
    noise = jax.random.normal(keys[3], (REPLICAS, LAYERS, INNER, WIDTH), jnp.float32)
    low = jnp.einsum('alir,lrw->aliw', left * strength, right[0])
    values = low * RANK ** (-0.5) + 0.5 * noise
    return jnp.clip(values, -6.0, 6.0).astype(jnp.bfloat16)


def block_levels(key, extent, cuts, least, largest):
    def one(position, blocks):
        steps = jax.random.uniform(jax.random.fold_in(jax.random.fold_in(key, 6), position), (blocks,), jnp.float32, least / len(cuts), largest / len(cuts))
        return jnp.repeat(jnp.exp(steps), extent[position] // blocks).reshape((-1,) + (1,) * (len(extent) - position - 1))

    gain = one(*cuts[0])
    for cut in cuts[1:]:
        gain = gain * one(*cut)
    return gain


def gaussian(stream_key, shape, scale, bound, cuts=(), held_as=jnp.bfloat16):
    values = jax.random.normal(stream_key, shape, jnp.float32) * scale
    if len(cuts) > 0:
        values = block_levels(stream_key, shape, cuts, -0.22, 0.18) * values
    return jnp.clip(values, min=-bound, max=bound).astype(held_as)


def setup_inputs(seed: int = 0) -> dict:
    arg_keys = jax.random.split(jax.random.key(seed), 5)
    gradients = draw_gradients(jax.random.fold_in(arg_keys[4], 71), 0)
    right_factor = gaussian(arg_keys[1], (LAYERS, WIDTH, RANK), 1.0, 6.0, (), jnp.float32)
    weights_before = gaussian(arg_keys[2], (LAYERS, INNER, WIDTH), WIDTH ** -0.5, 0.15625, ((1, 16), (2, 16)), jnp.float32)
    momentum = gaussian(arg_keys[3], (LAYERS, INNER, WIDTH), 0.05, 0.3125, ((1, 16), (2, 16)), jnp.float32)
    return {"gradients": gradients, "right_factor": right_factor, "weights_before": weights_before, "momentum": momentum}


def reference(gradients, right_factor, weights_before, momentum):
    small_basis = right_factor.astype(jnp.bfloat16)
    small_basis = lax.optimization_barrier(small_basis)
    left = jnp.einsum('aliw,lwr->lir', gradients.astype(jnp.float32), small_basis.astype(jnp.float32))
    gram = jnp.einsum('lir,lis->lrs', left, left, precision=lax.Precision.HIGHEST)
    gram = gram + 0.001 * lax.optimization_barrier(jnp.mean(jnp.diagonal(gram, axis1=1, axis2=2), axis=1))[:, None, None] * jnp.eye(RANK, dtype=jnp.float32)
    small_left = lax.optimization_barrier(left.astype(jnp.bfloat16))
    right = jnp.einsum('aliw,lir->lwr', gradients.astype(jnp.float32), small_left.astype(jnp.float32))
    root = jnp.linalg.cholesky(gram)
    half = lax.linalg.triangular_solve(root, jnp.swapaxes(right, 1, 2), left_side=True, lower=True)
    mixed = lax.linalg.triangular_solve(root, half, left_side=True, lower=True, transpose_a=True)
    change = jnp.einsum('lir,lrw->liw', left, mixed, precision=lax.Precision.HIGHEST) / REPLICAS
    new_momentum = 0.8 * momentum + change
    new_weights = weights_before - 0.05 * new_momentum
    new_basis = right * lax.rsqrt(lax.optimization_barrier(jnp.mean(right * right, axis=(1, 2), keepdims=True)) + 1e-12)
    return (new_weights, new_basis, new_momentum)
```

```python
import functools

import jax
import jax.numpy as jnp
from jax import lax
from jax.experimental import pallas as pl
from jax.experimental.pallas import tpu as pltpu
from jax.sharding import PartitionSpec as P

MESH = pl.DeviceIdType.MESH
F32 = jnp.float32
BF16 = jnp.bfloat16
HIGH = lax.Precision.HIGHEST

LAYERS = 4
RANK = 32
ROWS = 320
WIDTH = 1280
LANES = LAYERS * RANK
OWN = 80
ROW_PARTS = 1
PARTS = ((0, 2), (2, 3))


def nt_dot(a, b, precision=None):
    return lax.dot_general(
        a, b, (((1,), (1,)), ((), ())), precision=precision, preferred_element_type=F32
    )


def nn_dot(a, b, precision=None):
    return lax.dot_general(
        a, b, (((1,), (0,)), ((), ())), precision=precision, preferred_element_type=F32
    )


def tn_dot(a, b, precision=None):
    return lax.dot_general(
        a, b, (((0,), (0,)), ((), ())), precision=precision, preferred_element_type=F32
    )


def total_of(ref, count):
    value = ref[0]
    for i in range(1, count):
        value = value + ref[i]
    return value


def inverse_blocks(gram):
    row = lax.broadcasted_iota(jnp.int32, (RANK, LANES), 0)
    lane = lax.broadcasted_iota(jnp.int32, (RANK, LANES), 1)
    inner = lane % RANK
    group_r = lax.broadcasted_iota(jnp.int32, (LANES, LANES), 0) // RANK
    group_c = lax.broadcasted_iota(jnp.int32, (LANES, LANES), 1) // RANK
    same = (group_r == group_c).astype(F32)
    diagonal = jnp.where(row == inner, gram, 0.0)
    trace = jnp.sum(diagonal, axis=0, keepdims=True)
    mean = nn_dot(jnp.broadcast_to(trace, (8, LANES)), same, HIGH)[0:1] * (1.0 / RANK)
    a = gram + jnp.where(row == inner, 0.001 * mean, 0.0)
    for k in range(RANK):
        column = jnp.zeros_like(a)
        for l in range(LAYERS):
            at = l * RANK + k
            column = jnp.where(
                lane // RANK == l, jnp.broadcast_to(a[:, at : at + 1], a.shape), column
            )
        pivot = 1.0 / column[k : k + 1, :]
        here = inner == k
        new_row = jnp.where(here[0:1], 1.0, a[k : k + 1, :]) * pivot
        a = jnp.where(row == k, new_row, jnp.where(here, 0.0, a) - column * new_row)
    return a


def exchange(
    g_hbm, rt_hbm, right_out, pt_out,
    g_buf, r_buf, part_left, l1, l2, left_all, gr_src, gr_d2d, gr_yz, gr_full,
    pr, d2d, rs_src, rs, zr, ag, left_t,
    load_sem, l_send, l1_recv, l2_recv, l3_recv, gr_send, gr_recv,
    r_send, r1_recv, r2_recv, r3_recv, r4_recv, r5_recv, out_sem,
):
    d = lax.axis_index("dp")
    t = lax.axis_index("tp")
    x, zh = lax.rem(d, 4), lax.div(d, 4)
    zl, y, c = lax.div(t, 8), lax.rem(lax.div(t, 2), 4), lax.rem(t, 2)
    z = zh * 2 + zl
    chip = x * 4 + y
    yz = zl * 4 + y

    def device(x_, y_, z_, c_):
        return (lax.div(z_, 2) * 4 + x_, lax.rem(z_, 2) * 8 + y_ * 2 + c_)

    def shifted(value, step, size):
        return lax.rem(value + step, size)

    x_peers = [(shifted(x, k, 4), device(shifted(x, k, 4), y, z, c)) for k in (1, 3, 2)]
    zh_peers = [device(x, y, shifted(z, 2 * k, 8), c) for k in (1, 3, 2)]
    z_peers = [device(x, y, shifted(z, k, 8), c) for k in (4, 3, 5, 2, 6, 1, 7)]
    plane_peers = []
    for dx, dy in sorted(
        [(i, j) for i in range(4) for j in range(4) if i or j],
        key=lambda p: -(min(p[0], 4 - p[0]) + min(p[1], 4 - p[1])),
    ):
        x_, y_ = shifted(x, dx, 4), shifted(y, dy, 4)
        plane_peers.append((x_ * 4 + y_, device(x_, y_, z, c)))
    other_z = zh * 2 + (1 - zl)
    yz_peers = [device(x, shifted(y, k, 4), z, c) for k in (1, 2, 3)] + [
        device(x, shifted(y, k, 4), other_z, c) for k in (0, 1, 2, 3)
    ]
    partner = device(x, y, z, 1 - c)

    def send(src, dst, send_sem, recv_sem, to):
        pltpu.make_async_remote_copy(
            src_ref=src, dst_ref=dst, send_sem=send_sem, recv_sem=recv_sem,
            device_id=to, device_id_type=MESH,
        ).start()

    def take(ref, sem):
        pltpu.make_async_copy(ref, ref, sem).wait()

    loads = []
    for l in range(LAYERS):
        a = pltpu.make_async_copy(rt_hbm.at[l], r_buf.at[l], load_sem.at[l])
        b = pltpu.make_async_copy(g_hbm.at[l], g_buf.at[l], load_sem.at[LAYERS + l])
        a.start()
        b.start()
        loads.append((a, b))

    barrier = pltpu.get_barrier_semaphore()
    everyone = [p for _, p in plane_peers] + z_peers + yz_peers[4:] + [partner]
    for p in everyone:
        pl.semaphore_signal(barrier, inc=1, device_id=p, device_id_type=MESH)

    acc = None
    for l in range(LAYERS):
        for copy in loads[l]:
            copy.wait()
        pieces = []
        if l > 0:
            pieces.append(jnp.zeros((l * RANK, WIDTH), BF16))
        pieces.append(r_buf[l].astype(BF16))
        if l < LAYERS - 1:
            pieces.append(jnp.zeros(((LAYERS - 1 - l) * RANK, WIDTH), BF16))
        term = nt_dot(g_buf[l], jnp.concatenate(pieces, axis=0))
        acc = term if acc is None else acc + term
    part_left[...] = acc.reshape(4, ROWS // 4, LANES)

    pl.semaphore_wait(barrier, len(everyone))

    size = ROWS // 4 // ROW_PARTS
    for s in range(ROW_PARTS):
        rows = pl.ds(s * size, size)
        for n, (x_, p) in enumerate(x_peers):
            send(part_left.at[x_, rows], l1.at[x, rows], l_send.at[0], l1_recv.at[s], p)
    l1[x] = part_left[x]
    for s in range(ROW_PARTS):
        rows = pl.ds(s * size, size)
        take(l1.at[pl.ds(0, 3), rows], l1_recv.at[s])
        l2[zh, rows] = l1[0, rows] + l1[1, rows] + l1[2, rows] + l1[3, rows]
        for p in zh_peers:
            send(l2.at[zh, rows], l2.at[zh, rows], l_send.at[1], l2_recv.at[s], p)
    for s in range(ROW_PARTS):
        rows = pl.ds(s * size, size)
        take(l2.at[pl.ds(0, 3), rows], l2_recv.at[s])
        left_all[x, rows] = l2[0, rows] + l2[1, rows] + l2[2, rows] + l2[3, rows]
        for _, p in x_peers:
            send(left_all.at[x, rows], left_all.at[x, rows], l_send.at[2], l3_recv.at[s], p)
    for s in range(ROW_PARTS):
        rows = pl.ds(s * size, size)
        take(left_all.at[pl.ds(0, 3), rows], l3_recv.at[s])

    left = left_all[...].reshape(ROWS, LANES)
    turned = left.T
    left_t[...] = turned
    small = turned.astype(BF16)

    for n, (p0, m) in enumerate(PARTS):
        columns = slice(p0 * 256, (p0 + m) * 256)
        for l in range(LAYERS):
            term = nn_dot(small[l * RANK : (l + 1) * RANK], g_buf[l, :, columns])
            for i in range(2 * m):
                pr[p0 + i // 2, i % 2, l * RANK : (l + 1) * RANK] = term[
                    :, i * 128 : (i + 1) * 128
                ]
        span = pl.ds(p0, m)
        send(pr.at[span, 1 - c], d2d.at[span], r_send.at[0], r1_recv.at[n], partner)

    block = tn_dot(left, left, HIGH)
    lane = lax.broadcasted_iota(jnp.int32, (RANK, LANES), 1) // RANK
    compact = jnp.zeros((RANK, LANES), F32)
    for l in range(LAYERS):
        compact = jnp.where(lane == l, block[l * RANK : (l + 1) * RANK], compact)
    gr_src[...] = compact.reshape(2, RANK // 2, LANES)
    send(gr_src.at[1 - c], gr_d2d, gr_send.at[0], gr_recv.at[0], partner)

    for n, (p0, m) in enumerate(PARTS):
        span = pl.ds(p0, m)
        take(d2d.at[span], r1_recv.at[n])
        rs_src[span] = pr[span, c] + d2d[span]
        for i, p in plane_peers:
            send(
                rs_src.at[span, pl.ds(i * 8, 8)], rs.at[chip, span],
                r_send.at[1], r2_recv.at[n], p,
            )
        rs[chip, span] = rs_src[span, pl.ds(pl.multiple_of(chip * 8, 8), 8)]

    take(gr_d2d, gr_recv.at[0])
    gr_yz[yz] = gr_src[c] + gr_d2d[...]
    for p in yz_peers:
        send(gr_yz.at[yz], gr_yz.at[yz], gr_send.at[1], gr_recv.at[1], p)

    for n, (p0, m) in enumerate(PARTS):
        span = pl.ds(p0, m)
        take(rs.at[pl.ds(0, 15), span], r2_recv.at[n])
        value = rs[0, span]
        for i in range(1, 16):
            value = value + rs[i, span]
        zr[z, span] = value
        for p in z_peers:
            send(zr.at[z, span], zr.at[z, span], r_send.at[2], r3_recv.at[n], p)

    take(gr_yz.at[pl.ds(0, 7)], gr_recv.at[1])
    gr_full[c] = total_of(gr_yz, 8)
    send(gr_full.at[c], gr_full.at[c], gr_send.at[2], gr_recv.at[2], partner)

    mine = pl.ds(pl.multiple_of(chip * 8, 8), 8)
    for n, (p0, m) in enumerate(PARTS):
        span = pl.ds(p0, m)
        take(zr.at[pl.ds(0, 7), span], r3_recv.at[n])
        value = zr[0, span]
        for i in range(1, 8):
            value = value + zr[i, span]
        ag[span, c, mine] = value
        for _, p in plane_peers:
            send(
                ag.at[span, c, mine], ag.at[span, c, mine], r_send.at[3], r4_recv.at[n], p
            )

    take(gr_full.at[0], gr_recv.at[2])
    inverse = inverse_blocks(gr_full[...].reshape(RANK, LANES))
    spread = jnp.concatenate(
        [jnp.where(lane == l, inverse, 0.0) for l in range(LAYERS)], axis=0
    )
    pt_out[...] = nn_dot(spread, left_t[...], HIGH) * (1.0 / 16)

    outs = []
    for n, (p0, m) in enumerate(PARTS):
        span = pl.ds(p0, m)
        take(ag.at[span, 0, pl.ds(0, 120)], r4_recv.at[n])
        send(ag.at[span, c], ag.at[span, c], r_send.at[4], r5_recv.at[n], partner)
    for n, (p0, m) in enumerate(PARTS):
        span = pl.ds(p0, m)
        take(ag.at[span, 0], r5_recv.at[n])
        for p in range(p0, p0 + m):
            for h in range(2):
                right_out[:, (2 * p + h) * 128 : (2 * p + h + 1) * 128] = ag[p, h]

    for n in range(3):
        take(left_all.at[pl.ds(0, 3)], l_send.at[n])
    take(gr_src.at[0], gr_send.at[0])
    take(gr_yz.at[pl.ds(0, 7)], gr_send.at[1])
    take(gr_full.at[0], gr_send.at[2])
    take(pr.at[:, 0], r_send.at[0])
    take(rs.at[pl.ds(0, 15)], r_send.at[1])
    take(zr.at[pl.ds(0, 7)], r_send.at[2])
    take(rs.at[pl.ds(0, 15)], r_send.at[3])
    take(pr.at[:, 0], r_send.at[4])


def finish(right_ref, pt_ref, w_ref, m_ref, new_w_ref, new_b_ref, new_m_ref):
    d = lax.axis_index("dp")
    place = d * OWN
    first = jnp.minimum(lax.div(place, 128), WIDTH // 128 - 2)
    window = right_ref[:, pl.ds(pl.multiple_of(first * 128, 128), 256)]
    offset = place - first * 128
    own = pltpu.roll(window, lax.rem(256 - offset, 256), 1)[:, :128]
    turned = own.T[:OWN]
    lane = lax.broadcasted_iota(jnp.int32, (OWN, LANES), 1) // RANK
    stacked = jnp.concatenate(
        [jnp.where(lane == l, turned, 0.0) for l in range(LAYERS)], axis=0
    )
    change = nn_dot(stacked, pt_ref[...], HIGH)
    for l in range(LAYERS):
        new_m = 0.8 * m_ref[l] + change[l * OWN : (l + 1) * OWN]
        new_m_ref[l] = new_m
        new_w_ref[l] = w_ref[l] - 0.05 * new_m
        part = right_ref[l * RANK : (l + 1) * RANK]
        mean = jnp.sum(part * part) * (1.0 / (RANK * WIDTH))
        new_b_ref[l] = part * lax.rsqrt(jnp.full((1, 1), mean + 1e-12, F32))


def on_device(gradients, right_factor, weights_before, momentum):
    anywhere = pl.BlockSpec(memory_space=pl.ANY)
    vmem = pl.BlockSpec(memory_space=pltpu.VMEM)
    dma = pltpu.SemaphoreType.DMA
    parts = len(PARTS)
    right, pt = pl.pallas_call(
        exchange,
        out_shape=(
            jax.ShapeDtypeStruct((LANES, WIDTH), F32),
            jax.ShapeDtypeStruct((LANES, ROWS), F32),
        ),
        in_specs=[anywhere, anywhere],
        out_specs=[vmem, vmem],
        scratch_shapes=[
            pltpu.VMEM((LAYERS, ROWS, WIDTH), BF16),
            pltpu.VMEM((LAYERS, RANK, WIDTH), F32),
            pltpu.VMEM((4, ROWS // 4, LANES), F32),
            pltpu.VMEM((4, ROWS // 4, LANES), F32),
            pltpu.VMEM((4, ROWS // 4, LANES), F32),
            pltpu.VMEM((4, ROWS // 4, LANES), F32),
            pltpu.VMEM((2, RANK // 2, LANES), F32),
            pltpu.VMEM((RANK // 2, LANES), F32),
            pltpu.VMEM((8, RANK // 2, LANES), F32),
            pltpu.VMEM((2, RANK // 2, LANES), F32),
            pltpu.VMEM((5, 2, LANES, 128), F32),
            pltpu.VMEM((5, LANES, 128), F32),
            pltpu.VMEM((5, LANES, 128), F32),
            pltpu.VMEM((16, 5, 8, 128), F32),
            pltpu.VMEM((8, 5, 8, 128), F32),
            pltpu.VMEM((5, 2, LANES, 128), F32),
            pltpu.VMEM((LANES, ROWS), F32),
            dma((2 * LAYERS,)),
            dma((3,)),
            dma((ROW_PARTS,)),
            dma((ROW_PARTS,)),
            dma((ROW_PARTS,)),
            dma((3,)),
            dma((3,)),
            dma((5,)),
            dma((parts,)),
            dma((parts,)),
            dma((parts,)),
            dma((parts,)),
            dma((parts,)),
            dma((1,)),
        ],
        compiler_params=pltpu.CompilerParams(
            collective_id=0, has_side_effects=True, vmem_limit_bytes=32 << 20
        ),
        name="exchange",
    )(gradients[0], jnp.swapaxes(right_factor, 1, 2))
    new_w, new_b, new_m = pl.pallas_call(
        finish,
        out_shape=(
            jax.ShapeDtypeStruct((LAYERS, OWN, ROWS), F32),
            jax.ShapeDtypeStruct((LAYERS, RANK, WIDTH), F32),
            jax.ShapeDtypeStruct((LAYERS, OWN, ROWS), F32),
        ),
        in_specs=[vmem] * 4,
        out_specs=[vmem] * 3,
        name="finish",
        compiler_params=pltpu.CompilerParams(vmem_limit_bytes=24 << 20),
    )(right, pt, jnp.swapaxes(weights_before, 1, 2), jnp.swapaxes(momentum, 1, 2))
    return (
        jnp.swapaxes(new_w, 1, 2),
        jnp.swapaxes(new_b, 1, 2),
        jnp.swapaxes(new_m, 1, 2),
    )


def solution(mesh):
    return jax.shard_map(
        on_device,
        mesh=mesh,
        in_specs=(P("dp", None, "tp", None), P(), P(None, "tp", "dp"), P(None, "tp", "dp")),
        out_specs=(P(None, "tp", "dp"), P(), P(None, "tp", "dp")),
        check_vma=False,
    )
```
